32 devices in a mesh: tok: 2 (over x), blk: 16 (over z, y, core).
Axes of the slice: x: 2, y: 2, z: 4, core: 2. Of those that a mesh axis runs over, the one named last changes fastest.
Arguments:
- grad_out: bfloat16 [2048, 8192], P('tok', 'blk'), may hold values from -6 to 6
- acts: bfloat16 [2048, 512], P('tok', 'blk'), may hold values from -6 to 6
- stat_old: float32 [2, 16, 512, 512], P('tok', 'blk'), may hold values from -1 to 6, as said below
- root_old: float32 [2, 16, 512, 512], P('tok', 'blk'), may hold values from -1 to 2, as said below
- assign: int32 [16, 2], P('blk'), may hold values from 0 to 1, as said below
Outputs:
- roots: float32 [2, 16, 512, 512], P('tok', 'blk')
- precond: float32 [2, 16, 256, 512], P('tok', 'blk')
The draws below stay inside these ranges and needn't reach their ends.
Inputs may be any that keep to these rules, and one draw needn't show every extreme that they name: `assign`: row j gives each of its 2 slots a job 2 b + s with b < 1 and s in 0, 1; every job once in a row; slots 2 m and 2 m + 1 hold the two sides of one block. `stat_old`: each slot's matrix is symmetric and positive definite. `root_old`: each slot's matrix is symmetric.
All inputs are finite; a program needn't handle non-finite values.
Results may differ from the reference program's by a relative error of at most 0.0003.
Values may be sent and summed in bfloat16 or wider, within the bound.
No kernel may reach another device: no remote copies, remote signals or barrier semaphores. Data moves between devices by JAX's collectives and lax.ppermute only.
A program may use at most 64 MiB of HBM per device.

```python
import math
import jax
import jax.numpy as jnp
from jax import lax

DM = 8192
BS = 512
TOK_DEV = 1024
ITERS = 2
STRIPS = 16
GROUP_BLOCKS = 1
COLS = 512
TOKENS = 2048
N_TOK = 2
N_BLK = 16


def diagonal_scales(key):
    base = jax.random.fold_in(key, 11)
    logs = jax.random.uniform(base, (N_TOK, N_BLK, BS), jnp.float32, jnp.log(0.25), jnp.log(4.0))
    return jnp.exp(logs)


def older_scales(key):
    diagonal = diagonal_scales(key)
    base = jax.random.fold_in(key, 13)
    ageing = jax.random.uniform(base, (N_TOK, N_BLK, BS), jnp.float32, 1.0, 2.5)
    return diagonal * ageing


def symmetric_noise(key, salt):
    inner = jax.random.fold_in(key, salt)
    shape_full = (N_TOK, N_BLK, BS, BS)
    raw_noise = jax.random.normal(inner, shape_full, jnp.float32)
    identity = jnp.eye(BS, dtype=jnp.float32)
    return (raw_noise + jnp.swapaxes(raw_noise, -1, -2)) * 0.7071 * (1.0 - identity)


def draw_stat_old(key, part):
    diagonal = diagonal_scales(key)
    noise_part = symmetric_noise(key, 29)
    identity = jnp.eye(BS, dtype=jnp.float32)
    couple = jnp.sqrt(diagonal[..., :, None] * diagonal[..., None, :])
    return identity * diagonal[..., None] + 0.004 * couple * noise_part


def draw_root_old(key, part):
    diagonal = older_scales(key)
    noise_part = symmetric_noise(key, 37)
    identity = jnp.eye(BS, dtype=jnp.float32)
    couple = (diagonal[..., :, None] * diagonal[..., None, :]) ** (-0.125)
    return identity * (diagonal ** (-0.25))[..., None] + 0.002 * couple * noise_part


def draw_assign(key, part):
    pair_count = N_TOK // 2
    base = jax.random.fold_in(key, 23)
    order_keys = jax.random.split(jax.random.fold_in(base, 1), N_BLK)
    orders = jax.vmap(lambda inner: jax.random.permutation(inner, pair_count))(order_keys)
    flip_bits = jax.random.randint(jax.random.fold_in(base, 2), (N_BLK, pair_count), 0, 2)
    first_job = 2 * orders + flip_bits
    second_job = 2 * orders + 1 - flip_bits
    return jnp.stack([first_job, second_job], axis=-1).reshape(N_BLK, N_TOK).astype(jnp.int32)


def steps_of(key, dims, pieces, smallest, high):
    level, own = 1.0, jax.random.fold_in(key, 6)
    for axis_at, parts in pieces:
        heights = jnp.exp(jax.random.uniform(jax.random.fold_in(own, axis_at), (parts,), jnp.float32, smallest / len(pieces), high / len(pieces)))
        level = level * jnp.repeat(heights, dims[axis_at] // parts).reshape([-1 if axis == axis_at else 1 for axis in range(len(dims))])
    return level


def gaussian(stream_key, shape, scale, limit, pieces=(), held_as=jnp.bfloat16):
    array = scale * jax.random.normal(stream_key, shape, jnp.float32)
    if pieces:
        array = array * steps_of(stream_key, shape, pieces, -0.22, 0.18)
    return jnp.clip(array, -limit, limit).astype(held_as)


def setup_inputs(seed: int = 0) -> dict:
    splits = jax.random.split(jax.random.key(seed), 6)
    grad_out = gaussian(splits[0], (TOKENS, DM), 1.0, 6.0, ((0, 2), (1, 16)))
    acts = gaussian(splits[1], (TOKENS, COLS), 1.0, 6.0, ((0, 2), (1, 16)))
    stat_old = draw_stat_old(jax.random.fold_in(splits[5], 71), 0)
    root_old = draw_root_old(jax.random.fold_in(splits[5], 71), 0)
    assign = draw_assign(jax.random.fold_in(splits[5], 71), 0)
    return {"grad_out": grad_out, "acts": acts, "stat_old": stat_old, "root_old": root_old, "assign": assign}


BETA = 0.9
DAMPING = 0.001

def product(lhs_matrix, rhs_matrix):
    return jnp.dot(lhs_matrix, rhs_matrix, precision=lax.Precision.HIGHEST, preferred_element_type=jnp.float32)

def newton_root(statistic, warm_root, square):
    identity = jnp.eye(square.shape[0], dtype=jnp.float32)
    factor = BETA * statistic + (1.0 - BETA) * square + DAMPING * identity
    root_square = product(warm_root, warm_root)
    coupled = product(product(root_square, root_square), factor)
    current = warm_root
    for iteration in range(ITERS):
        update = (5.0 * identity - coupled) * 0.25
        current = product(current, update)
        if iteration + 1 < ITERS:
            update_square = product(update, update)
            coupled = product(product(update_square, update_square), coupled)
    return current

def reference(grad_out, acts, stat_old, root_old, assign):
    group_width = GROUP_BLOCKS * BS
    scaling = 1.0 / math.sqrt(TOKENS)
    shard_cols = DM // N_BLK
    strided = grad_out.reshape(TOKENS, N_BLK // STRIPS, STRIPS, shard_cols)

    def per_column(column):
        strip_index = (column % STRIPS).astype(jnp.int32)
        col_start = (column // STRIPS * group_width).astype(jnp.int32)
        rows_part = lax.dynamic_slice_in_dim(strided, strip_index, 1, 2).reshape(TOKENS, BS)
        rows_part = rows_part.astype(jnp.float32).reshape(N_TOK, TOK_DEV, BS)
        cols_part = lax.dynamic_slice_in_dim(acts, col_start, group_width, 1).astype(jnp.float32).reshape(N_TOK, TOK_DEV, group_width)
        partial_value = jnp.einsum('ktr,ktc->krc', rows_part, cols_part, precision=lax.Precision.HIGHEST) * scaling
        gradient = lax.optimization_barrier(jnp.sum(partial_value, axis=0))
        blocks = gradient.reshape(BS, GROUP_BLOCKS, BS).transpose(1, 0, 2)
        job_table = assign[column]

        def per_slot(position):
            job_index = job_table[position]
            chosen = blocks[job_index // 2]
            oriented = jnp.where(job_index % 2 == 0, chosen, chosen.T)
            square = product(oriented, oriented.T) / TOKENS
            return newton_root(stat_old[position, column], root_old[position, column], square)
        root_stack = lax.map(per_slot, jnp.arange(N_TOK, dtype=jnp.int32))

        def per_output(position):
            job_index = job_table[position]
            side_bit = job_index % 2
            chosen = blocks[job_index // 2]
            own_root = root_stack[position]
            other_root = root_stack[jnp.bitwise_xor(position, 1)]
            left_root = jnp.where(side_bit == 0, own_root, other_root)
            right_root = jnp.where(side_bit == 0, other_root, own_root)
            half_rows = lax.dynamic_slice_in_dim(left_root, (side_bit * (BS // 2)).astype(jnp.int32), BS // 2, 0)
            return product(product(half_rows, chosen), right_root)
        return (root_stack, lax.map(per_output, jnp.arange(N_TOK, dtype=jnp.int32)))
    root_stack, precond = lax.map(per_column, jnp.arange(N_BLK, dtype=jnp.int32))
    return (root_stack.transpose(1, 0, 2, 3), precond.transpose(1, 0, 2, 3))
```

```python
import math

import jax
import jax.numpy as jnp
from jax import lax
from jax.sharding import PartitionSpec as P

ITERS = 2


BETA = 0.9
DAMPING = 0.001


def swapped(block, axis, stride):
    count = lax.axis_size(axis)
    route = []
    for low in range(count):
        high = low | 1 << stride
        if high != low and high < count:
            route += [(low, high), (high, low)]
    return lax.ppermute(block, axis, route)


def shortened(x):
    return jax.tree.map(lambda a: a.astype(jnp.bfloat16) if a.dtype == jnp.float32 else a, x)


def product(lhs_matrix, rhs_matrix):
    return jnp.dot(
        lhs_matrix, rhs_matrix, precision=lax.Precision.HIGH, preferred_element_type=jnp.float32
    )


def newton_root(statistic, warm_root, square):
    identity = jnp.eye(square.shape[0], dtype=jnp.float32)
    factor = BETA * statistic + (1.0 - BETA) * square + DAMPING * identity
    root_square = product(warm_root, warm_root)
    coupled = product(product(root_square, root_square), factor)
    current = warm_root
    for iteration in range(ITERS):
        update = (5.0 * identity - coupled) * 0.25
        current = product(current, update)
        if iteration + 1 < ITERS:
            update_square = product(update, update)
            coupled = product(product(update_square, update_square), coupled)
    return current


def block_partials(rows_part, cols_part, group_blocks, block_size, scaling):
    shaped = cols_part.reshape(cols_part.shape[0], group_blocks, block_size)
    return (
        jnp.einsum("tr,tgc->grc", rows_part, shaped, preferred_element_type=jnp.float32) * scaling
    )


def join_pair(mine, theirs, column, bit):
    lower = column // (1 << bit) % 2 == 0
    return jnp.where(
        lower, jnp.concatenate([mine, theirs], axis=0), jnp.concatenate([theirs, mine], axis=0)
    )


def shards(grad_out, acts, stat_old, root_old, assign):
    token_groups = lax.axis_size("tok")
    blk_count = lax.axis_size("blk")
    column = lax.axis_index("blk")
    position = lax.axis_index("tok")
    block_size = stat_old.shape[-1]
    shard_rows = grad_out.shape[0]
    all_tokens = shard_rows * token_groups
    scaling = 1.0 / math.sqrt(all_tokens)
    strips = grad_out.shape[1] * blk_count // block_size
    strip_bits = strips.bit_length() - 1
    blk_bits = blk_count.bit_length() - 1
    group_blocks = token_groups // 2
    cols_part = acts.T
    for bit in reversed(range(strip_bits)):
        other_cols = swapped(cols_part, "blk", bit)
        cols_part = join_pair(cols_part, other_cols, column, bit)
    cols_part = cols_part.reshape((2,) * strip_bits + acts.shape[::-1])
    cols_part = cols_part.transpose(tuple(reversed(range(strip_bits))) + (strip_bits, strip_bits + 1))
    cols_part = cols_part.reshape(-1, shard_rows).T
    rows_part = grad_out
    for bit in range(strip_bits, blk_bits):
        other_rows = swapped(shortened(rows_part), "blk", bit).astype(rows_part.dtype)
        rows_part = join_pair(rows_part.T, other_rows.T, column, bit).T
    job_table = assign[0]
    job_index = job_table[position]
    side_bit = job_index % 2
    partial_value = block_partials(rows_part, cols_part, group_blocks, block_size, scaling)
    if token_groups == 2:
        chosen = (partial_value + swapped(partial_value, "tok", 0))[0]
    else:
        halves = partial_value.reshape(group_blocks * 2, block_size // 2, block_size)[job_table]
        own_half = lax.psum_scatter(halves, "tok", scatter_dimension=0, tiled=True)[0]
        other_half = swapped(own_half, "tok", 0)
        chosen = jnp.where(
            side_bit == 0,
            jnp.concatenate([own_half, other_half], axis=0),
            jnp.concatenate([other_half, own_half], axis=0),
        )
    oriented = jnp.where(side_bit == 0, chosen, chosen.T)
    square = product(oriented, oriented.T) / all_tokens
    own_root = newton_root(stat_old[0, 0], root_old[0, 0], square)
    other_root = swapped(own_root, "tok", 0)
    left_root = jnp.where(side_bit == 0, own_root, other_root)
    right_root = jnp.where(side_bit == 0, other_root, own_root)
    half_rows = lax.dynamic_slice_in_dim(
        left_root, side_bit * (block_size // 2), block_size // 2, 0
    )
    precond = product(product(half_rows, chosen), right_root)
    return (own_root[None, None], precond[None, None])


def solution(mesh):
    placed = (
        P("tok", "blk"),
        P("tok", "blk"),
        P("tok", "blk", None, None),
        P("tok", "blk", None, None),
        P("blk", None),
    )
    return jax.shard_map(
        shards,
        mesh=mesh,
        in_specs=placed,
        out_specs=(P("tok", "blk", None, None), P("tok", "blk", None, None)),
        check_vma=False,
    )
```

```python
import functools
import math

import jax
import jax.numpy as jnp
from jax import lax
from jax.experimental import pallas as pl
from jax.experimental.pallas import tpu as pltpu
from jax.sharding import PartitionSpec as P

ITERS = 2


BETA = 0.9
DAMPING = 0.001
TAIL = 16
GRANT = 24 << 20


def swapped(block, axis, stride):
    return moved(block, axis, 1 << stride)


def moved(block, axis, mask):
    count = lax.axis_size(axis)
    return lax.ppermute(block, axis, [(low, low ^ mask) for low in range(count) if low ^ mask < count])


def product(lhs_matrix, rhs_matrix):
    return jnp.dot(
        lhs_matrix, rhs_matrix, precision=lax.Precision.HIGH, preferred_element_type=jnp.float32
    )


def newton_root(statistic, warm_root, square):
    identity = jnp.eye(square.shape[0], dtype=jnp.float32)
    factor = BETA * statistic + (1.0 - BETA) * square + DAMPING * identity
    root_square = product(warm_root, warm_root)
    coupled = product(product(root_square, root_square), factor)
    current = warm_root
    for iteration in range(ITERS):
        update = (5.0 * identity - coupled) * 0.25
        current = product(current, update)
        if iteration + 1 < ITERS:
            update_square = product(update, update)
            coupled = product(product(update_square, update_square), coupled)
    return current


def block_partials(rows_part, cols_part, group_blocks, block_size, scaling):
    shaped = cols_part.reshape(cols_part.shape[0], group_blocks, block_size)
    return (
        jnp.einsum("tr,tgc->grc", rows_part, shaped, preferred_element_type=jnp.float32) * scaling
    )


def join_pair(mine, theirs, column, bit):
    lower = column // (1 << bit) % 2 == 0
    return jnp.where(
        lower, jnp.concatenate([mine, theirs], axis=1), jnp.concatenate([theirs, mine], axis=1)
    )


def general(grad_out, acts, stat_old, root_old, assign):
    token_groups = lax.axis_size("tok")
    blk_count = lax.axis_size("blk")
    column = lax.axis_index("blk")
    position = lax.axis_index("tok")
    block_size = stat_old.shape[-1]
    shard_rows = grad_out.shape[0]
    all_tokens = shard_rows * token_groups
    scaling = 1.0 / math.sqrt(all_tokens)
    strips = grad_out.shape[1] * blk_count // block_size
    strip_bits = strips.bit_length() - 1
    blk_bits = blk_count.bit_length() - 1
    group_blocks = token_groups // 2
    cols_part = acts
    for bit in range(strip_bits):
        other_cols = swapped(cols_part, "blk", bit)
        cols_part = join_pair(cols_part, other_cols, column, bit)
    rows_part = grad_out
    for bit in range(strip_bits, blk_bits):
        other_rows = swapped(rows_part, "blk", bit)
        rows_part = join_pair(rows_part, other_rows, column, bit)
    job_table = assign[0]
    job_index = job_table[position]
    side_bit = job_index % 2
    partial_value = block_partials(rows_part, cols_part, group_blocks, block_size, scaling)
    halves = partial_value.reshape(group_blocks * 2, block_size // 2, block_size)[job_table]
    own_half = lax.psum_scatter(halves, "tok", scatter_dimension=0, tiled=True)[0]
    other_half = swapped(own_half, "tok", 0)
    chosen = jnp.where(
        side_bit == 0,
        jnp.concatenate([own_half, other_half], axis=0),
        jnp.concatenate([other_half, own_half], axis=0),
    )
    oriented = jnp.where(side_bit == 0, chosen, chosen.T)
    square = product(oriented, oriented.T) / all_tokens
    own_root = newton_root(stat_old[0, 0], root_old[0, 0], square)
    other_root = swapped(own_root, "tok", 0)
    left_root = jnp.where(side_bit == 0, own_root, other_root)
    right_root = jnp.where(side_bit == 0, other_root, own_root)
    half_rows = lax.dynamic_slice_in_dim(
        left_root, side_bit * (block_size // 2), block_size // 2, 0
    )
    precond = product(product(half_rows, chosen), right_root)
    return (own_root[None, None], precond[None, None])


def split(value):
    high = value.astype(jnp.bfloat16)
    return high, (value - high.astype(jnp.float32)).astype(jnp.bfloat16)


def multiply(lhs, rhs, dims=((1,), (0,))):
    def one(a, b):
        return lax.dot_general(a, b, (dims, ((), ())), preferred_element_type=jnp.float32)

    return one(lhs[0], rhs[0]) + (one(lhs[0], rhs[1]) + one(lhs[1], rhs[0]))


def exponent_of(value):
    largest = jnp.max(jnp.abs(value), axis=0, keepdims=True)
    return jnp.clip(jnp.ceil(jnp.log2(jnp.maximum(largest, 1e-30))), -100.0, 100.0)


def side_of(assign_ref):
    return assign_ref[0, lax.axis_index("tok")] % 2


def eye_mask(rows, cols):
    return lax.broadcasted_iota(jnp.int32, (rows, cols), 0) == lax.broadcasted_iota(
        jnp.int32, (rows, cols), 1
    )


def partial_body(*refs, scaling, pieces):
    grad_ref, own_ref, pay_ref, held_ref = refs[pieces:]
    part_rows = refs[0].shape[0]
    for index in range(pieces):
        held_ref[index * part_rows : (index + 1) * part_rows, :] = refs[index][...]
    own = jnp.dot(held_ref[...], grad_ref[...], preferred_element_type=jnp.float32) * scaling
    own_ref[...] = own
    power = exponent_of(own)
    rows = own.shape[0]
    pay_ref[0:rows, :] = own * jnp.exp2(-power)
    pay_ref[rows:, :] = jnp.broadcast_to(power, (TAIL, own.shape[1]))


def partial_chunk(parts, grad, scaling):
    rows = sum(part.shape[0] for part in parts)
    width = grad.shape[1]
    return call(
        functools.partial(partial_body, scaling=scaling, pieces=len(parts)),
        [((rows, width), jnp.float32), ((rows + TAIL, width), jnp.float32)],
        "partial",
        [*parts, grad],
        [pltpu.VMEM((rows, grad.shape[0]), grad.dtype)],
    )


def fourth_body(root_ref, out_ref):
    first = split(root_ref[...])
    second = split(multiply(first, first))
    out_ref[...] = multiply(second, second)


def root_body(*refs, groups, all_tokens):
    assign_ref = refs[0]
    count = len(groups)
    stat_ref, warm_ref, fourth_ref = refs[1 + 2 * count : 4 + 2 * count]
    root_ref, pay_ref, high_ref, low_ref, held_ref = refs[4 + 2 * count :]
    column, side = lax.axis_index("blk"), side_of(assign_ref)
    size = stat_ref.shape[-1]
    for group, masks in enumerate(groups):
        own_ref, got_ref = refs[1 + 2 * group : 3 + 2 * group]
        rows = own_ref.shape[0]
        part_rows = rows // len(masks)
        scale = jnp.exp2(got_ref[rows : rows + 1, :])
        for index, mask in enumerate(masks):
            span = slice(index * part_rows, (index + 1) * part_rows)
            target = pl.multiple_of((column ^ mask) * part_rows, part_rows)
            held_ref[pl.ds(target, part_rows), :] = own_ref[span, :] + got_ref[span, :] * scale

    @pl.when(side == 0)
    def _():
        held_ref[...] = held_ref[...].T

    oriented = split(held_ref[...])
    high_ref[...] = oriented[0]
    low_ref[...] = oriented[1]
    square = multiply(oriented, oriented, ((1,), (1,))) * (1.0 / all_tokens)
    identity = jnp.where(eye_mask(size, size), 1.0, 0.0)
    factor = BETA * stat_ref[...] + (1.0 - BETA) * square + DAMPING * identity
    coupled = multiply(split(fourth_ref[...]), split(factor))
    current = warm_ref[...]
    for iteration in range(ITERS):
        update = split((5.0 * identity - coupled) * 0.25)
        current = multiply(split(current), update)
        if iteration + 1 < ITERS:
            update_square = split(multiply(update, update))
            coupled = multiply(split(multiply(update_square, update_square)), split(coupled))
    root_ref[...] = current
    power = exponent_of(current)
    scaled = current * jnp.exp2(-power)
    diagonal = jnp.sum(scaled * identity, axis=0, keepdims=True)
    coarse = jnp.round(diagonal * 1024.0) * (1.0 / 1024.0)
    pay_ref[0:size, :] = scaled * (1.0 - identity)
    row = lax.broadcasted_iota(jnp.int32, (TAIL, size), 0)
    tail = jnp.where(row == 0, power, jnp.where(row == 1, coarse, diagonal - coarse))
    pay_ref[size:, :] = tail


def middle_body(assign_ref, root_ref, high_ref, low_ref, out_ref):
    half = root_ref.shape[0] // 2
    oriented = high_ref[...], low_ref[...]

    @pl.when(side_of(assign_ref) == 0)
    def _():
        out_ref[0:half, :] = multiply(split(root_ref[0:half, :]), oriented)
        out_ref[half:, :] = jnp.zeros((half, root_ref.shape[1]), jnp.float32)

    @pl.when(side_of(assign_ref) != 0)
    def _():
        out_ref[...] = multiply(oriented, split(root_ref[...]), ((0,), (0,)))


def final_body(assign_ref, got_ref, middle_ref, out_ref):
    size = middle_ref.shape[0]
    half = size // 2
    scale = jnp.exp2(got_ref[size : size + 1, :])
    diagonal = got_ref[size + 1 : size + 2, :] + got_ref[size + 2 : size + 3, :]
    other = jnp.where(eye_mask(size, size), diagonal, got_ref[0:size, :]) * scale

    @pl.when(side_of(assign_ref) == 0)
    def _():
        out_ref[...] = multiply(split(middle_ref[0:half, :]), split(other))

    @pl.when(side_of(assign_ref) != 0)
    def _():
        out_ref[...] = multiply(split(other[half:, :]), split(middle_ref[...]))


def call(body, shapes, name, operands, scratch=()):
    smem = pl.BlockSpec(memory_space=pltpu.SMEM)
    vmem = pl.BlockSpec(memory_space=pltpu.VMEM)
    whole = [operand.dtype == jnp.int32 for operand in operands]
    operands = [
        operand if scalar else pltpu.with_memory_space_constraint(operand, pltpu.VMEM)
        for operand, scalar in zip(operands, whole)
    ]
    return pl.pallas_call(
        body,
        out_shape=tuple(pltpu.VMEM(*shape) for shape in shapes),
        in_specs=[smem if scalar else vmem for scalar in whole],
        out_specs=tuple(vmem for _ in shapes),
        scratch_shapes=list(scratch),
        name=name,
        compiler_params=pltpu.CompilerParams(vmem_limit_bytes=GRANT),
    )(*operands)


def paired(grad_out, acts, stat_old, root_old, assign):
    blk_count = lax.axis_size("blk")
    size = stat_old.shape[-1]
    all_tokens = grad_out.shape[0] * lax.axis_size("tok")
    scaling = 1.0 / math.sqrt(all_tokens)
    square = (size, size)
    parts = {0: acts.T}
    far = [mask for mask in range(4, blk_count, 4)]
    for mask in reversed(far):
        parts[mask] = moved(parts[0], "blk", mask)
    parts[2] = moved(parts[0], "blk", 2)
    for mask in far:
        parts[mask | 2] = moved(parts[mask], "blk", 2)
    early = [0, 2] + far
    late = [mask | 2 for mask in far]
    groups = []
    for masks in (early, late):
        for mask in masks:
            parts[mask | 1] = moved(parts[mask], "blk", 1)
        groups.append(masks + [mask | 1 for mask in masks])
    warm = root_old[0, 0]
    (fourth,) = call(fourth_body, [(square, jnp.float32)], "fourth", [warm])
    operands = [assign]
    for masks in groups:
        own, pay = partial_chunk([parts[mask] for mask in masks], grad_out, scaling)
        got = moved(pay.astype(jnp.float16), "tok", 1).astype(jnp.float32)
        operands += [own, got]
    own_root, pay, high, low = call(
        functools.partial(root_body, groups=groups, all_tokens=all_tokens),
        [
            (square, jnp.float32),
            ((size + TAIL, size), jnp.float32),
            (square, jnp.bfloat16),
            (square, jnp.bfloat16),
        ],
        "root",
        operands + [stat_old[0, 0], warm, fourth],
        [pltpu.VMEM(square, jnp.float32)],
    )
    got = moved(pay.astype(jnp.float16), "tok", 1).astype(jnp.float32)
    (middle,) = call(
        middle_body, [(square, jnp.float32)], "middle", [assign, own_root, high, low]
    )
    (precond,) = call(
        final_body, [((size // 2, size), jnp.float32)], "final", [assign, got, middle]
    )
    return (own_root[None, None], precond[None, None])


def shards(grad_out, acts, stat_old, root_old, assign):
    blk_count = lax.axis_size("blk")
    strips = grad_out.shape[1] * blk_count // stat_old.shape[-1]
    plain = lax.axis_size("tok") == 2 and strips == blk_count and blk_count % 8 == 0
    body = paired if plain and acts.shape[1] % 32 == 0 else general
    return body(grad_out, acts, stat_old, root_old, assign)


def solution(mesh):
    placed = (
        P("tok", "blk"),
        P("tok", "blk"),
        P("tok", "blk", None, None),
        P("tok", "blk", None, None),
        P("blk", None),
    )
    return jax.shard_map(
        shards,
        mesh=mesh,
        in_specs=placed,
        out_specs=(P("tok", "blk", None, None), P("tok", "blk", None, None)),
        check_vma=False,
    )
```

```python
import functools
import math

import jax
import jax.numpy as jnp
from jax import lax
from jax.experimental import pallas as pl
from jax.experimental.pallas import tpu as pltpu
from jax.sharding import PartitionSpec as P


ITERS = 2


BETA = 0.9
DAMPING = 0.001
TAIL = 8
GRANT = 24 << 20


def swapped(block, axis, stride):
    return moved(block, axis, 1 << stride)


def crossed(block, mask):
    half = lax.axis_size("blk")
    return lax.ppermute(
        block, ("tok", "blk"), [(low, low ^ half ^ mask) for low in range(2 * half)]
    )


def moved(block, axis, mask):
    count = lax.axis_size(axis)
    return lax.ppermute(block, axis, [(low, low ^ mask) for low in range(count) if low ^ mask < count])


def product(lhs_matrix, rhs_matrix):
    return jnp.dot(
        lhs_matrix, rhs_matrix, precision=lax.Precision.HIGH, preferred_element_type=jnp.float32
    )


def newton_root(statistic, warm_root, square):
    identity = jnp.eye(square.shape[0], dtype=jnp.float32)
    factor = BETA * statistic + (1.0 - BETA) * square + DAMPING * identity
    root_square = product(warm_root, warm_root)
    coupled = product(product(root_square, root_square), factor)
    current = warm_root
    for iteration in range(ITERS):
        update = (5.0 * identity - coupled) * 0.25
        current = product(current, update)
        if iteration + 1 < ITERS:
            update_square = product(update, update)
            coupled = product(product(update_square, update_square), coupled)
    return current


def block_partials(rows_part, cols_part, group_blocks, block_size, scaling):
    shaped = cols_part.reshape(cols_part.shape[0], group_blocks, block_size)
    return (
        jnp.einsum("tr,tgc->grc", rows_part, shaped, preferred_element_type=jnp.float32) * scaling
    )


def join_pair(mine, theirs, column, bit):
    lower = column // (1 << bit) % 2 == 0
    return jnp.where(
        lower, jnp.concatenate([mine, theirs], axis=1), jnp.concatenate([theirs, mine], axis=1)
    )


def general(grad_out, acts, stat_old, root_old, assign):
    token_groups = lax.axis_size("tok")
    blk_count = lax.axis_size("blk")
    column = lax.axis_index("blk")
    position = lax.axis_index("tok")
    block_size = stat_old.shape[-1]
    shard_rows = grad_out.shape[0]
    all_tokens = shard_rows * token_groups
    scaling = 1.0 / math.sqrt(all_tokens)
    strips = grad_out.shape[1] * blk_count // block_size
    strip_bits = strips.bit_length() - 1
    blk_bits = blk_count.bit_length() - 1
    group_blocks = token_groups // 2
    cols_part = acts
    for bit in range(strip_bits):
        other_cols = swapped(cols_part, "blk", bit)
        cols_part = join_pair(cols_part, other_cols, column, bit)
    rows_part = grad_out
    for bit in range(strip_bits, blk_bits):
        other_rows = swapped(rows_part, "blk", bit)
        rows_part = join_pair(rows_part, other_rows, column, bit)
    job_table = assign[0]
    job_index = job_table[position]
    side_bit = job_index % 2
    partial_value = block_partials(rows_part, cols_part, group_blocks, block_size, scaling)
    halves = partial_value.reshape(group_blocks * 2, block_size // 2, block_size)[job_table]
    own_half = lax.psum_scatter(halves, "tok", scatter_dimension=0, tiled=True)[0]
    other_half = swapped(own_half, "tok", 0)
    chosen = jnp.where(
        side_bit == 0,
        jnp.concatenate([own_half, other_half], axis=0),
        jnp.concatenate([other_half, own_half], axis=0),
    )
    oriented = jnp.where(side_bit == 0, chosen, chosen.T)
    square = product(oriented, oriented.T) / all_tokens
    own_root = newton_root(stat_old[0, 0], root_old[0, 0], square)
    other_root = swapped(own_root, "tok", 0)
    left_root = jnp.where(side_bit == 0, own_root, other_root)
    right_root = jnp.where(side_bit == 0, other_root, own_root)
    half_rows = lax.dynamic_slice_in_dim(
        left_root, side_bit * (block_size // 2), block_size // 2, 0
    )
    precond = product(product(half_rows, chosen), right_root)
    return (own_root[None, None], precond[None, None])


def split(value):
    high = value.astype(jnp.bfloat16)
    return high, (value - high.astype(jnp.float32)).astype(jnp.bfloat16)


def multiply(lhs, rhs, dims=((1,), (0,))):
    def one(a, b):
        return lax.dot_general(a, b, (dims, ((), ())), preferred_element_type=jnp.float32)

    return one(lhs[0], rhs[0]) + (one(lhs[0], rhs[1]) + one(lhs[1], rhs[0]))


def exponent_of(value):
    largest = jnp.max(jnp.abs(value), axis=0, keepdims=True)
    return jnp.clip(jnp.ceil(jnp.log2(jnp.maximum(largest, 1e-30))), -100.0, 100.0)


def side_of(assign_ref):
    return assign_ref[0, lax.axis_index("tok")] % 2


def eye_mask(rows, cols):
    return lax.broadcasted_iota(jnp.int32, (rows, cols), 0) == lax.broadcasted_iota(
        jnp.int32, (rows, cols), 1
    )


def partial_body(*refs, scaling, pieces):
    grad_refs = refs[pieces : pieces + 2]
    outs = refs[pieces + 2 :]
    held_ref = outs[-1]
    part_rows = refs[0].shape[0]
    rows = pieces * part_rows
    for index in range(pieces):
        held_ref[index * part_rows : (index + 1) * part_rows, :] = refs[index][...]
    for which, grad_ref in enumerate(grad_refs):
        own_ref, pay_ref = outs[2 * which : 2 * which + 2]
        own = jnp.dot(held_ref[...], grad_ref[...], preferred_element_type=jnp.float32) * scaling
        own_ref[...] = own
        power = exponent_of(own)
        pay_ref[0:rows, :] = own * jnp.exp2(-power)
        pay_ref[rows:, :] = jnp.broadcast_to(power, (TAIL, own.shape[1]))


def partial_chunk(parts, grads, scaling):
    rows = sum(part.shape[0] for part in parts)
    width = grads[0].shape[1]
    return call(
        functools.partial(partial_body, scaling=scaling, pieces=len(parts)),
        [((rows, width), jnp.float32), ((rows + TAIL, width), jnp.float32)] * 2,
        [*parts, *grads],
        [pltpu.VMEM((rows, grads[0].shape[0]), grads[0].dtype)],
    )


def stage_body(*refs):
    count = len(refs) // 2
    copies = [
        pltpu.make_async_copy(refs[index], refs[count + index], refs[-1].at[index])
        for index in range(count)
    ]
    for copy in copies:
        copy.start()
    for copy in copies:
        copy.wait()


def stage(operands):
    operands = [pltpu.with_memory_space_constraint(operand, pltpu.HBM) for operand in operands]
    return pl.pallas_call(
        stage_body,
        out_shape=tuple(pltpu.VMEM(operand.shape, operand.dtype) for operand in operands),
        in_specs=[pl.BlockSpec(memory_space=pl.ANY) for _ in operands],
        out_specs=tuple(pl.BlockSpec(memory_space=pltpu.VMEM) for _ in operands),
        scratch_shapes=[pltpu.SemaphoreType.DMA((len(operands),))],
        name="stage",
        compiler_params=pltpu.CompilerParams(vmem_limit_bytes=GRANT),
    )(*operands)


def squared_body(root_ref, out_ref):
    value = split(root_ref[...])
    out_ref[...] = multiply(value, value)


def root_body(*refs, groups, all_tokens):
    assign_ref = refs[0]
    count = len(groups)
    stat_ref, warm_ref, fourth_ref = refs[1 + 2 * count : 4 + 2 * count]
    root_ref, pay_ref, high_ref, low_ref, held_ref = refs[4 + 2 * count :]
    column, side = lax.axis_index("blk"), side_of(assign_ref)
    size = stat_ref.shape[-1]
    for group, masks in enumerate(groups):
        own_ref, got_ref = refs[1 + 2 * group : 3 + 2 * group]
        rows = own_ref.shape[0]
        part_rows = rows // len(masks)
        scale = jnp.exp2(got_ref[rows : rows + 1, :])
        for index, mask in enumerate(masks):
            span = slice(index * part_rows, (index + 1) * part_rows)
            target = pl.multiple_of((column ^ mask) * part_rows, part_rows)
            held_ref[pl.ds(target, part_rows), :] = own_ref[span, :] + got_ref[span, :] * scale

    @pl.when(side == 0)
    def _():
        held_ref[...] = held_ref[...].T

    oriented = split(held_ref[...])
    high_ref[...] = oriented[0]
    low_ref[...] = oriented[1]
    square = multiply(oriented, oriented, ((1,), (1,))) * (1.0 / all_tokens)
    identity = jnp.where(eye_mask(size, size), 1.0, 0.0)
    factor = BETA * stat_ref[...] + (1.0 - BETA) * square + DAMPING * identity
    coupled = multiply(split(fourth_ref[...]), split(factor))
    current = warm_ref[...]
    for iteration in range(ITERS):
        update = split((5.0 * identity - coupled) * 0.25)
        current = multiply(split(current), update)
        if iteration + 1 < ITERS:
            update_square = split(multiply(update, update))
            coupled = multiply(split(multiply(update_square, update_square)), split(coupled))
    root_ref[...] = current
    power = exponent_of(current)
    scaled = current * jnp.exp2(-power)
    diagonal = jnp.sum(scaled * identity, axis=0, keepdims=True)
    coarse = jnp.round(diagonal * 1024.0) * (1.0 / 1024.0)
    pay_ref[0:size, :] = scaled * (1.0 - identity)
    row = lax.broadcasted_iota(jnp.int32, (TAIL, size), 0)
    tail = jnp.where(row == 0, power, jnp.where(row == 1, coarse, diagonal - coarse))
    pay_ref[size:, :] = tail


def middle_body(assign_ref, root_ref, high_ref, low_ref, out_ref):
    half = root_ref.shape[0] // 2
    oriented = high_ref[...], low_ref[...]

    @pl.when(side_of(assign_ref) == 0)
    def _():
        out_ref[0:half, :] = multiply(split(root_ref[0:half, :]), oriented)
        out_ref[half:, :] = jnp.zeros((half, root_ref.shape[1]), jnp.float32)

    @pl.when(side_of(assign_ref) != 0)
    def _():
        out_ref[...] = multiply(oriented, split(root_ref[...]), ((0,), (0,)))


def final_body(assign_ref, got_ref, middle_ref, out_ref):
    size = middle_ref.shape[0]
    half = size // 2
    scale = jnp.exp2(got_ref[size : size + 1, :])
    diagonal = got_ref[size + 1 : size + 2, :] + got_ref[size + 2 : size + 3, :]
    other = jnp.where(eye_mask(size, size), diagonal, got_ref[0:size, :]) * scale

    @pl.when(side_of(assign_ref) == 0)
    def _():
        out_ref[...] = multiply(split(middle_ref[0:half, :]), split(other))

    @pl.when(side_of(assign_ref) != 0)
    def _():
        out_ref[...] = multiply(split(other[half:, :]), split(middle_ref[...]))


def call(body, shapes, operands, scratch=()):
    smem = pl.BlockSpec(memory_space=pltpu.SMEM)
    vmem = pl.BlockSpec(memory_space=pltpu.VMEM)
    whole = [operand.dtype == jnp.int32 for operand in operands]
    operands = [
        operand if scalar else pltpu.with_memory_space_constraint(operand, pltpu.VMEM)
        for operand, scalar in zip(operands, whole)
    ]
    return pl.pallas_call(
        body,
        out_shape=tuple(pltpu.VMEM(*shape) for shape in shapes),
        in_specs=[smem if scalar else vmem for scalar in whole],
        out_specs=tuple(vmem for _ in shapes),
        scratch_shapes=list(scratch),
        compiler_params=pltpu.CompilerParams(vmem_limit_bytes=GRANT),
    )(*operands)


def paired(grad_out, acts, stat_old, root_old, assign):
    blk_count = lax.axis_size("blk")
    size = stat_old.shape[-1]
    all_tokens = grad_out.shape[0] * lax.axis_size("tok")
    scaling = 1.0 / math.sqrt(all_tokens)
    square = (size, size)
    far = [mask for mask in range(4, blk_count, 4)]
    sent = acts.T
    parts = {}
    for mask in reversed([2] + far):
        parts[mask] = moved(sent, "blk", mask)
    parts[0], grad, warm, stat = stage([sent, grad_out, root_old[0, 0], stat_old[0, 0]])
    for mask in far:
        parts[mask | 2] = moved(parts[mask], "blk", 2)
    grads = [grad, moved(grad_out, "blk", 1)]
    (second,) = call(squared_body, [(square, jnp.float32)], [warm])
    (fourth,) = call(squared_body, [(square, jnp.float32)], [second])
    groups = []
    operands = [assign]
    for masks in ([0, 2] + far[:1], far[1:], [mask | 2 for mask in far]):
        own, own_pay, beside, beside_pay = partial_chunk(
            [parts[mask] for mask in masks], grads, scaling
        )
        own_pay, beside_pay = own_pay.astype(jnp.float16), beside_pay.astype(jnp.float16)
        got, got_beside = crossed(own_pay, 0), crossed(beside_pay, 1)
        beside = moved(beside, "blk", 1)
        operands += [own, got.astype(jnp.float32), beside, got_beside.astype(jnp.float32)]
        groups += [masks, [mask | 1 for mask in masks]]
    own_root, pay, high, low = call(
        functools.partial(root_body, groups=groups, all_tokens=all_tokens),
        [
            (square, jnp.float32),
            ((size + TAIL, size), jnp.float32),
            (square, jnp.bfloat16),
            (square, jnp.bfloat16),
        ],
        operands + [stat, warm, fourth],
        [pltpu.VMEM(square, jnp.float32)],
    )
    got = moved(pay.astype(jnp.float16), "tok", 1).astype(jnp.float32)
    (middle,) = call(middle_body, [(square, jnp.float32)], [assign, own_root, high, low])
    (precond,) = call(final_body, [((size // 2, size), jnp.float32)], [assign, got, middle])
    return (own_root[None, None], precond[None, None])


def is_paired(mesh_shape, rows, size, features):
    strips = rows // size
    plain = mesh_shape["tok"] == 2 and strips == mesh_shape["blk"] and strips % 8 == 0
    return plain and features % (32 * strips) == 0


def solution(mesh):
    placed = (
        P("tok", "blk"),
        P("tok", "blk"),
        P("tok", "blk", None, None),
        P("tok", "blk", None, None),
        P("blk", None),
    )

    def whole(grad_out, acts, stat_old, root_old, assign):
        fast = is_paired(mesh.shape, grad_out.shape[1], stat_old.shape[-1], acts.shape[1])

        def shards(*args):
            return (paired if fast else general)(*args)

        mapped = jax.shard_map(
            shards,
            mesh=mesh,
            in_specs=placed,
            out_specs=(P("tok", "blk", None, None), P("tok", "blk", None, None)),
            check_vma=False,
        )
        return mapped(grad_out, acts, stat_old, root_old, assign)

    return whole
```

```python
import functools
import math

import jax
import jax.numpy as jnp
from jax import lax
from jax.experimental import pallas as pl
from jax.experimental.pallas import tpu as pltpu
from jax.sharding import PartitionSpec as P


ITERS = 2


BETA = 0.9
DAMPING = 0.001
TAIL = 8
GRANT = 24 << 20


def swapped(block, axis, stride):
    return moved(block, axis, 1 << stride)


def crossed(block, mask):
    half = lax.axis_size("blk")
    return lax.ppermute(
        block, ("tok", "blk"), [(low, low ^ half ^ mask) for low in range(2 * half)]
    )


def moved(block, axis, mask):
    count = lax.axis_size(axis)
    return lax.ppermute(block, axis, [(low, low ^ mask) for low in range(count) if low ^ mask < count])


def product(lhs_matrix, rhs_matrix):
    return jnp.dot(
        lhs_matrix, rhs_matrix, precision=lax.Precision.HIGH, preferred_element_type=jnp.float32
    )


def newton_root(statistic, warm_root, square):
    identity = jnp.eye(square.shape[0], dtype=jnp.float32)
    factor = BETA * statistic + (1.0 - BETA) * square + DAMPING * identity
    root_square = product(warm_root, warm_root)
    coupled = product(product(root_square, root_square), factor)
    current = warm_root
    for iteration in range(ITERS):
        update = (5.0 * identity - coupled) * 0.25
        current = product(current, update)
        if iteration + 1 < ITERS:
            update_square = product(update, update)
            coupled = product(product(update_square, update_square), coupled)
    return current


def block_partials(rows_part, cols_part, group_blocks, block_size, scaling):
    shaped = cols_part.reshape(cols_part.shape[0], group_blocks, block_size)
    return (
        jnp.einsum("tr,tgc->grc", rows_part, shaped, preferred_element_type=jnp.float32) * scaling
    )


def join_pair(mine, theirs, column, bit):
    lower = column // (1 << bit) % 2 == 0
    return jnp.where(
        lower, jnp.concatenate([mine, theirs], axis=1), jnp.concatenate([theirs, mine], axis=1)
    )


def general(grad_out, acts, stat_old, root_old, assign):
    token_groups = lax.axis_size("tok")
    blk_count = lax.axis_size("blk")
    column = lax.axis_index("blk")
    position = lax.axis_index("tok")
    block_size = stat_old.shape[-1]
    shard_rows = grad_out.shape[0]
    all_tokens = shard_rows * token_groups
    scaling = 1.0 / math.sqrt(all_tokens)
    strips = grad_out.shape[1] * blk_count // block_size
    strip_bits = strips.bit_length() - 1
    blk_bits = blk_count.bit_length() - 1
    group_blocks = token_groups // 2
    cols_part = acts
    for bit in range(strip_bits):
        other_cols = swapped(cols_part, "blk", bit)
        cols_part = join_pair(cols_part, other_cols, column, bit)
    rows_part = grad_out
    for bit in range(strip_bits, blk_bits):
        other_rows = swapped(rows_part, "blk", bit)
        rows_part = join_pair(rows_part, other_rows, column, bit)
    job_table = assign[0]
    job_index = job_table[position]
    side_bit = job_index % 2
    partial_value = block_partials(rows_part, cols_part, group_blocks, block_size, scaling)
    halves = partial_value.reshape(group_blocks * 2, block_size // 2, block_size)[job_table]
    own_half = lax.psum_scatter(halves, "tok", scatter_dimension=0, tiled=True)[0]
    other_half = swapped(own_half, "tok", 0)
    chosen = jnp.where(
        side_bit == 0,
        jnp.concatenate([own_half, other_half], axis=0),
        jnp.concatenate([other_half, own_half], axis=0),
    )
    oriented = jnp.where(side_bit == 0, chosen, chosen.T)
    square = product(oriented, oriented.T) / all_tokens
    own_root = newton_root(stat_old[0, 0], root_old[0, 0], square)
    other_root = swapped(own_root, "tok", 0)
    left_root = jnp.where(side_bit == 0, own_root, other_root)
    right_root = jnp.where(side_bit == 0, other_root, own_root)
    half_rows = lax.dynamic_slice_in_dim(
        left_root, side_bit * (block_size // 2), block_size // 2, 0
    )
    precond = product(product(half_rows, chosen), right_root)
    return (own_root[None, None], precond[None, None])


def split(value):
    high = value.astype(jnp.bfloat16)
    return high, (value - high.astype(jnp.float32)).astype(jnp.bfloat16)


def multiply(lhs, rhs, dims=((1,), (0,))):
    def one(a, b):
        return lax.dot_general(a, b, (dims, ((), ())), preferred_element_type=jnp.float32)

    return one(lhs[0], rhs[0]) + (one(lhs[0], rhs[1]) + one(lhs[1], rhs[0]))


def exponent_of(value):
    largest = jnp.max(jnp.abs(value), axis=0, keepdims=True)
    return jnp.clip(jnp.ceil(jnp.log2(jnp.maximum(largest, 1e-30))), -100.0, 100.0)


def side_of(assign_ref):
    return assign_ref[0, lax.axis_index("tok")] % 2


def eye_mask(rows, cols):
    return lax.broadcasted_iota(jnp.int32, (rows, cols), 0) == lax.broadcasted_iota(
        jnp.int32, (rows, cols), 1
    )


def partial_body(*refs, scaling, pieces):
    grad_refs = refs[pieces : pieces + 2]
    outs = refs[pieces + 2 :]
    held_ref = outs[-1]
    part_rows = refs[0].shape[0]
    rows = pieces * part_rows
    for index in range(pieces):
        held_ref[index * part_rows : (index + 1) * part_rows, :] = refs[index][...]
    for which, grad_ref in enumerate(grad_refs):
        own_ref, pay_ref = outs[2 * which : 2 * which + 2]
        own = jnp.dot(held_ref[...], grad_ref[...], preferred_element_type=jnp.float32) * scaling
        own_ref[...] = own
        power = exponent_of(own)
        pay_ref[0:rows, :] = own * jnp.exp2(-power)
        pay_ref[rows:, :] = jnp.broadcast_to(power, (TAIL, own.shape[1]))


def partial_chunk(parts, grads, scaling):
    rows = sum(part.shape[0] for part in parts)
    width = grads[0].shape[1]
    return call(
        functools.partial(partial_body, scaling=scaling, pieces=len(parts)),
        [((rows, width), jnp.float32), ((rows + TAIL, width), jnp.float32)] * 2,
        [*parts, *grads],
        [pltpu.VMEM((rows, grads[0].shape[0]), grads[0].dtype)],
    )


def stage_body(*refs):
    count = len(refs) // 2
    copies = [
        pltpu.make_async_copy(refs[index], refs[count + index], refs[-1].at[index])
        for index in range(count)
    ]
    for copy in copies:
        copy.start()
    for copy in copies:
        copy.wait()


def stage(operands):
    operands = [pltpu.with_memory_space_constraint(operand, pltpu.HBM) for operand in operands]
    return pl.pallas_call(
        stage_body,
        out_shape=tuple(pltpu.VMEM(operand.shape, operand.dtype) for operand in operands),
        in_specs=[pl.BlockSpec(memory_space=pl.ANY) for _ in operands],
        out_specs=tuple(pl.BlockSpec(memory_space=pltpu.VMEM) for _ in operands),
        scratch_shapes=[pltpu.SemaphoreType.DMA((len(operands),))],
        name="stage",
        compiler_params=pltpu.CompilerParams(vmem_limit_bytes=GRANT),
    )(*operands)


def mark_body(block_ref, out_ref):
    out_ref[...] = block_ref[0:8, 0:128].astype(jnp.float32)


def mark(block):
    return call(mark_body, [((8, 128), jnp.float32)], [block])


def fourth_body(assign_ref, root_ref, early_ref, late_ref, out_ref):
    value = split(root_ref[...])
    value = split(multiply(value, value))
    out_ref[...] = multiply(value, value)


def root_body(*refs, groups, all_tokens):
    assign_ref = refs[0]
    count = len(groups)
    stat_ref, warm_ref, fourth_ref = refs[1 + 2 * count : 4 + 2 * count]
    root_ref, top_ref, bottom_ref, high_ref, low_ref, held_ref = refs[4 + 2 * count :]
    column, side = lax.axis_index("blk"), side_of(assign_ref)
    size = stat_ref.shape[-1]
    for group, masks in enumerate(groups):
        own_ref, got_ref = refs[1 + 2 * group : 3 + 2 * group]
        rows = own_ref.shape[0]
        part_rows = rows // len(masks)
        scale = jnp.exp2(got_ref[rows : rows + 1, :])
        for index, mask in enumerate(masks):
            span = slice(index * part_rows, (index + 1) * part_rows)
            target = pl.multiple_of((column ^ mask) * part_rows, part_rows)
            held_ref[pl.ds(target, part_rows), :] = own_ref[span, :] + got_ref[span, :] * scale

    @pl.when(side == 0)
    def _():
        held_ref[...] = held_ref[...].T

    oriented = split(held_ref[...])
    high_ref[...] = oriented[0]
    low_ref[...] = oriented[1]
    square = multiply(oriented, oriented, ((1,), (1,))) * (1.0 / all_tokens)
    identity = jnp.where(eye_mask(size, size), 1.0, 0.0)
    factor = BETA * stat_ref[...] + (1.0 - BETA) * square + DAMPING * identity
    coupled = multiply(split(fourth_ref[...]), split(factor))
    update = (5.0 * identity - coupled) * 0.25
    parts = split(update)
    update_square = multiply(parts, parts)
    parts = split(update_square)
    update_fourth = split(multiply(parts, parts))
    inner = split(4.0 * update_square - 5.0 * update)
    both_steps = (5.0 * update + multiply(update_fourth, inner)) * 0.25
    current = multiply(split(warm_ref[...]), split(both_steps))
    root_ref[...] = current
    power = exponent_of(current)
    scaled = current * jnp.exp2(-power)
    diagonal = jnp.sum(scaled * identity, axis=0, keepdims=True)
    coarse = jnp.round(diagonal * 1024.0) * (1.0 / 1024.0)
    half = size // 2
    scaled = scaled * (1.0 - identity)
    top_ref[...] = scaled[:half, :]
    bottom_ref[0:half, :] = scaled[half:, :]
    row = lax.broadcasted_iota(jnp.int32, (TAIL, size), 0)
    tail = jnp.where(row == 0, power, jnp.where(row == 1, coarse, diagonal - coarse))
    bottom_ref[half:, :] = tail


def middle_body(assign_ref, root_ref, high_ref, low_ref, out_ref):
    half = root_ref.shape[0] // 2
    oriented = high_ref[...], low_ref[...]

    @pl.when(side_of(assign_ref) == 0)
    def _():
        out_ref[0:half, :] = multiply(split(root_ref[0:half, :]), oriented)
        out_ref[half:, :] = jnp.zeros((half, root_ref.shape[1]), jnp.float32)

    @pl.when(side_of(assign_ref) != 0)
    def _():
        out_ref[...] = multiply(oriented, split(root_ref[...]), ((0,), (0,)))


def decoded(rows, tail, offset):
    mask = lax.broadcasted_iota(jnp.int32, rows.shape, 0) + offset == lax.broadcasted_iota(
        jnp.int32, rows.shape, 1
    )
    return jnp.where(mask, tail[1:2, :] + tail[2:3, :], rows) * jnp.exp2(tail[0:1, :])


def bottom_body(assign_ref, got_ref, middle_ref, out_ref, tail_ref):
    half = middle_ref.shape[0] // 2
    tail = got_ref[half:, :]
    tail_ref[...] = tail
    other = split(decoded(got_ref[0:half, :], tail, half))

    @pl.when(side_of(assign_ref) == 0)
    def _():
        out_ref[...] = multiply(split(middle_ref[0:half, half:]), other)

    @pl.when(side_of(assign_ref) != 0)
    def _():
        out_ref[...] = multiply(other, split(middle_ref[...]))


def top_body(assign_ref, got_ref, tail_ref, middle_ref, begun_ref, out_ref):
    half = middle_ref.shape[0] // 2

    @pl.when(side_of(assign_ref) == 0)
    def _():
        other = split(decoded(got_ref[...], tail_ref[...], 0))
        out_ref[...] = begun_ref[...] + multiply(split(middle_ref[0:half, 0:half]), other)

    @pl.when(side_of(assign_ref) != 0)
    def _():
        out_ref[...] = begun_ref[...]


def call(body, shapes, operands, scratch=(), kept=True):
    smem = pl.BlockSpec(memory_space=pltpu.SMEM)
    vmem = pl.BlockSpec(memory_space=pltpu.VMEM)
    whole = [operand.dtype == jnp.int32 for operand in operands]
    operands = [
        operand if scalar else pltpu.with_memory_space_constraint(operand, pltpu.VMEM)
        for operand, scalar in zip(operands, whole)
    ]
    return pl.pallas_call(
        body,
        out_shape=tuple((pltpu.VMEM if kept else jax.ShapeDtypeStruct)(*shape) for shape in shapes),
        in_specs=[smem if scalar else vmem for scalar in whole],
        out_specs=tuple(vmem for _ in shapes),
        scratch_shapes=list(scratch),
        compiler_params=pltpu.CompilerParams(vmem_limit_bytes=GRANT),
    )(*operands)


def paired(grad_out, acts, stat_old, root_old, assign):
    blk_count = lax.axis_size("blk")
    size = stat_old.shape[-1]
    all_tokens = grad_out.shape[0] * lax.axis_size("tok")
    scaling = 1.0 / math.sqrt(all_tokens)
    square = (size, size)
    far = [mask for mask in range(4, blk_count, 4)]
    sent = acts.T
    parts = {}
    for mask in reversed([2] + far):
        parts[mask] = moved(sent, "blk", mask)
    parts[0], grad, warm, stat = stage([sent, grad_out, root_old[0, 0], stat_old[0, 0]])
    for mask in far:
        parts[mask | 2] = moved(parts[mask], "blk", 2)
    grads = [grad, moved(grad_out, "blk", 1)]
    marks = mark(parts[0]) + mark(grads[0])
    (fourth,) = call(fourth_body, [(square, jnp.float32)], [assign, warm, *marks])
    groups = []
    operands = [assign]
    for masks in ([0, 2] + far[:1], far[1:] + [far[0] | 2], [mask | 2 for mask in far[1:]]):
        own, own_pay, beside, beside_pay = partial_chunk(
            [parts[mask] for mask in masks], grads, scaling
        )
        own_pay, beside_pay = own_pay.astype(jnp.float16), beside_pay.astype(jnp.float16)
        got, got_beside = crossed(own_pay, 0), crossed(beside_pay, 1)
        beside = moved(beside, "blk", 1)
        operands += [own, got.astype(jnp.float32), beside, got_beside.astype(jnp.float32)]
        groups += [masks, [mask | 1 for mask in masks]]
    half = size // 2
    own_root, top, bottom, high, low = call(
        functools.partial(root_body, groups=groups, all_tokens=all_tokens),
        [
            (square, jnp.float32),
            ((half, size), jnp.float32),
            ((half + TAIL, size), jnp.float32),
            (square, jnp.bfloat16),
            (square, jnp.bfloat16),
        ],
        operands + [stat, warm, fourth],
        [pltpu.VMEM(square, jnp.float32)],
    )
    bottom = crossed(bottom.astype(jnp.float16), 0)
    top = crossed(top.astype(jnp.float16), 0)
    (middle,) = call(middle_body, [(square, jnp.float32)], [assign, own_root, high, low])
    begun, tail = call(
        bottom_body,
        [((half, size), jnp.float32), ((TAIL, size), jnp.float32)],
        [assign, bottom.astype(jnp.float32), middle],
    )
    (precond,) = call(
        top_body,
        [((half, size), jnp.float32)],
        [assign, top.astype(jnp.float32), tail, middle, begun],
        kept=False,
    )
    return (own_root[None, None], precond[None, None])


def is_paired(mesh_shape, rows, size, features):
    strips = rows // size
    plain = mesh_shape["tok"] == 2 and strips == mesh_shape["blk"] and strips % 8 == 0
    return plain and features % (32 * strips) == 0


def solution(mesh):
    placed = (
        P("tok", "blk"),
        P("tok", "blk"),
        P("tok", "blk", None, None),
        P("tok", "blk", None, None),
        P("blk", None),
    )

    def whole(grad_out, acts, stat_old, root_old, assign):
        fast = is_paired(mesh.shape, grad_out.shape[1], stat_old.shape[-1], acts.shape[1])

        def shards(*args):
            return (paired if fast else general)(*args)

        mapped = jax.shard_map(
            shards,
            mesh=mesh,
            in_specs=placed,
            out_specs=(P("tok", "blk", None, None), P("tok", "blk", None, None)),
            check_vma=False,
        )
        return mapped(grad_out, acts, stat_old, root_old, assign)

    return whole
```

```python
import functools
import math

import jax
import jax.numpy as jnp
from jax import lax
from jax.experimental import pallas as pl
from jax.experimental.pallas import tpu as pltpu
from jax.sharding import PartitionSpec as P


ITERS = 2


BETA = 0.9
DAMPING = 0.001
TAIL = 8
GRANT = 24 << 20


def swapped(block, axis, stride):
    return moved(block, axis, 1 << stride)


def crossed(block, mask):
    half = lax.axis_size("blk")
    return lax.ppermute(
        block, ("tok", "blk"), [(low, low ^ half ^ mask) for low in range(2 * half)]
    )


def moved(block, axis, mask):
    count = lax.axis_size(axis)
    return lax.ppermute(block, axis, [(low, low ^ mask) for low in range(count) if low ^ mask < count])


def product(lhs_matrix, rhs_matrix):
    return jnp.dot(
        lhs_matrix, rhs_matrix, precision=lax.Precision.HIGH, preferred_element_type=jnp.float32
    )


def newton_root(statistic, warm_root, square):
    identity = jnp.eye(square.shape[0], dtype=jnp.float32)
    factor = BETA * statistic + (1.0 - BETA) * square + DAMPING * identity
    root_square = product(warm_root, warm_root)
    coupled = product(product(root_square, root_square), factor)
    current = warm_root
    for iteration in range(ITERS):
        update = (5.0 * identity - coupled) * 0.25
        current = product(current, update)
        if iteration + 1 < ITERS:
            update_square = product(update, update)
            coupled = product(product(update_square, update_square), coupled)
    return current


def block_partials(rows_part, cols_part, group_blocks, block_size, scaling):
    shaped = cols_part.reshape(cols_part.shape[0], group_blocks, block_size)
    return (
        jnp.einsum("tr,tgc->grc", rows_part, shaped, preferred_element_type=jnp.float32) * scaling
    )


def join_pair(mine, theirs, column, bit):
    lower = column // (1 << bit) % 2 == 0
    return jnp.where(
        lower, jnp.concatenate([mine, theirs], axis=1), jnp.concatenate([theirs, mine], axis=1)
    )


def general(grad_out, acts, stat_old, root_old, assign):
    token_groups = lax.axis_size("tok")
    blk_count = lax.axis_size("blk")
    column = lax.axis_index("blk")
    position = lax.axis_index("tok")
    block_size = stat_old.shape[-1]
    shard_rows = grad_out.shape[0]
    all_tokens = shard_rows * token_groups
    scaling = 1.0 / math.sqrt(all_tokens)
    strips = grad_out.shape[1] * blk_count // block_size
    strip_bits = strips.bit_length() - 1
    blk_bits = blk_count.bit_length() - 1
    group_blocks = token_groups // 2
    cols_part = acts
    for bit in range(strip_bits):
        other_cols = swapped(cols_part, "blk", bit)
        cols_part = join_pair(cols_part, other_cols, column, bit)
    rows_part = grad_out
    for bit in range(strip_bits, blk_bits):
        other_rows = swapped(rows_part, "blk", bit)
        rows_part = join_pair(rows_part, other_rows, column, bit)
    job_table = assign[0]
    job_index = job_table[position]
    side_bit = job_index % 2
    partial_value = block_partials(rows_part, cols_part, group_blocks, block_size, scaling)
    halves = partial_value.reshape(group_blocks * 2, block_size // 2, block_size)[job_table]
    own_half = lax.psum_scatter(halves, "tok", scatter_dimension=0, tiled=True)[0]
    other_half = swapped(own_half, "tok", 0)
    chosen = jnp.where(
        side_bit == 0,
        jnp.concatenate([own_half, other_half], axis=0),
        jnp.concatenate([other_half, own_half], axis=0),
    )
    oriented = jnp.where(side_bit == 0, chosen, chosen.T)
    square = product(oriented, oriented.T) / all_tokens
    own_root = newton_root(stat_old[0, 0], root_old[0, 0], square)
    other_root = swapped(own_root, "tok", 0)
    left_root = jnp.where(side_bit == 0, own_root, other_root)
    right_root = jnp.where(side_bit == 0, other_root, own_root)
    half_rows = lax.dynamic_slice_in_dim(
        left_root, side_bit * (block_size // 2), block_size // 2, 0
    )
    precond = product(product(half_rows, chosen), right_root)
    return (own_root[None, None], precond[None, None])


def split(value):
    high = value.astype(jnp.bfloat16)
    return high, (value - high.astype(jnp.float32)).astype(jnp.bfloat16)


def multiply(lhs, rhs, dims=((1,), (0,))):
    def one(a, b):
        return lax.dot_general(a, b, (dims, ((), ())), preferred_element_type=jnp.float32)

    return one(lhs[0], rhs[0]) + (one(lhs[0], rhs[1]) + one(lhs[1], rhs[0]))


def exponent_of(value):
    largest = jnp.max(jnp.abs(value), axis=0, keepdims=True)
    return jnp.clip(jnp.ceil(jnp.log2(jnp.maximum(largest, 1e-30))), -100.0, 100.0)


def side_of(assign_ref):
    return assign_ref[0, lax.axis_index("tok")] % 2


def eye_mask(rows, cols):
    return lax.broadcasted_iota(jnp.int32, (rows, cols), 0) == lax.broadcasted_iota(
        jnp.int32, (rows, cols), 1
    )


def partial_body(*refs, scaling, pieces):
    grad_refs = refs[pieces : pieces + 2]
    outs = refs[pieces + 2 :]
    held_ref = outs[-1]
    part_rows = refs[0].shape[0]
    rows = pieces * part_rows
    for index in range(pieces):
        held_ref[index * part_rows : (index + 1) * part_rows, :] = refs[index][...]
    for which, grad_ref in enumerate(grad_refs):
        own_ref, pay_ref = outs[2 * which : 2 * which + 2]
        own = jnp.dot(held_ref[...], grad_ref[...], preferred_element_type=jnp.float32) * scaling
        own_ref[...] = own
        power = exponent_of(own)
        pay_ref[0:rows, :] = own * jnp.exp2(-power)
        pay_ref[rows:, :] = jnp.broadcast_to(power, (TAIL, own.shape[1]))


def partial_chunk(parts, grads, scaling):
    rows = sum(part.shape[0] for part in parts)
    width = grads[0].shape[1]
    return call(
        functools.partial(partial_body, scaling=scaling, pieces=len(parts)),
        [((rows, width), jnp.float32), ((rows + TAIL, width), jnp.float32)] * 2,
        [*parts, *grads],
        [pltpu.VMEM((rows, grads[0].shape[0]), grads[0].dtype)],
    )


def stage_body(*refs):
    count = len(refs) // 2
    copies = [
        pltpu.make_async_copy(refs[index], refs[count + index], refs[-1].at[index])
        for index in range(count)
    ]
    for copy in copies:
        copy.start()
    for copy in copies:
        copy.wait()


def stage(operands):
    operands = [pltpu.with_memory_space_constraint(operand, pltpu.HBM) for operand in operands]
    return pl.pallas_call(
        stage_body,
        out_shape=tuple(pltpu.VMEM(operand.shape, operand.dtype) for operand in operands),
        in_specs=[pl.BlockSpec(memory_space=pl.ANY) for _ in operands],
        out_specs=tuple(pl.BlockSpec(memory_space=pltpu.VMEM) for _ in operands),
        scratch_shapes=[pltpu.SemaphoreType.DMA((len(operands),))],
        compiler_params=pltpu.CompilerParams(vmem_limit_bytes=GRANT),
    )(*operands)


def mark_body(block_ref, out_ref):
    out_ref[...] = block_ref[0:8, 0:128].astype(jnp.float32)


def mark(block):
    return call(mark_body, [((8, 128), jnp.float32)], [block])


def squared_body(root_ref, out_ref):
    value = split(root_ref[...])
    out_ref[...] = multiply(value, value)


def fourth_body(assign_ref, squared_ref, early_ref, out_ref):
    value = split(squared_ref[...])
    out_ref[...] = multiply(value, value)


def root_body(*refs, groups, all_tokens):
    assign_ref = refs[0]
    count = len(groups)
    stat_ref, warm_ref, fourth_ref = refs[1 + 2 * count : 4 + 2 * count]
    root_ref, top_ref, bottom_ref, high_ref, low_ref, held_ref = refs[4 + 2 * count :]
    column, side = lax.axis_index("blk"), side_of(assign_ref)
    size = stat_ref.shape[-1]
    for group, masks in enumerate(groups):
        own_ref, got_ref = refs[1 + 2 * group : 3 + 2 * group]
        rows = own_ref.shape[0]
        part_rows = rows // len(masks)
        scale = jnp.exp2(got_ref[rows : rows + 1, :])
        for index, mask in enumerate(masks):
            span = slice(index * part_rows, (index + 1) * part_rows)
            target = pl.multiple_of((column ^ mask) * part_rows, part_rows)
            held_ref[pl.ds(target, part_rows), :] = own_ref[span, :] + got_ref[span, :] * scale

    @pl.when(side == 0)
    def _():
        held_ref[...] = held_ref[...].T

    oriented = split(held_ref[...])
    high_ref[...] = oriented[0]
    low_ref[...] = oriented[1]
    square = multiply(oriented, oriented, ((1,), (1,))) * (1.0 / all_tokens)
    identity = jnp.where(eye_mask(size, size), 1.0, 0.0)
    factor = BETA * stat_ref[...] + (1.0 - BETA) * square + DAMPING * identity
    coupled = multiply(split(fourth_ref[...]), split(factor))
    update = (5.0 * identity - coupled) * 0.25
    parts = split(update)
    update_square = multiply(parts, parts)
    parts = split(update_square)
    update_fourth = split(multiply(parts, parts))
    inner = split(4.0 * update_square - 5.0 * update)
    both_steps = (5.0 * update + multiply(update_fourth, inner)) * 0.25
    current = multiply(split(warm_ref[...]), split(both_steps))
    root_ref[...] = current
    power = exponent_of(current)
    scaled = current * jnp.exp2(-power)
    diagonal = jnp.sum(scaled * identity, axis=0, keepdims=True)
    coarse = jnp.round(diagonal * 1024.0) * (1.0 / 1024.0)
    half = size // 2
    scaled = scaled * (1.0 - identity)
    top_ref[...] = scaled[:half, :]
    bottom_ref[0:half, :] = scaled[half:, :]
    row = lax.broadcasted_iota(jnp.int32, (TAIL, size), 0)
    tail = jnp.where(row == 0, power, jnp.where(row == 1, coarse, diagonal - coarse))
    bottom_ref[half:, :] = tail


def middle_body(assign_ref, root_ref, high_ref, low_ref, out_ref):
    half = root_ref.shape[0] // 2
    oriented = high_ref[...], low_ref[...]

    @pl.when(side_of(assign_ref) == 0)
    def _():
        out_ref[0:half, :] = multiply(split(root_ref[0:half, :]), oriented)
        out_ref[half:, :] = jnp.zeros((half, root_ref.shape[1]), jnp.float32)

    @pl.when(side_of(assign_ref) != 0)
    def _():
        out_ref[...] = multiply(oriented, split(root_ref[...]), ((0,), (0,)))


def decoded(rows, tail, offset):
    mask = lax.broadcasted_iota(jnp.int32, rows.shape, 0) + offset == lax.broadcasted_iota(
        jnp.int32, rows.shape, 1
    )
    return jnp.where(mask, tail[1:2, :] + tail[2:3, :], rows) * jnp.exp2(tail[0:1, :])


def bottom_body(assign_ref, got_ref, middle_ref, out_ref, tail_ref):
    half = middle_ref.shape[0] // 2
    tail = got_ref[half:, :]
    tail_ref[...] = tail
    other = split(decoded(got_ref[0:half, :], tail, half))

    @pl.when(side_of(assign_ref) == 0)
    def _():
        out_ref[...] = multiply(split(middle_ref[0:half, half:]), other)

    @pl.when(side_of(assign_ref) != 0)
    def _():
        out_ref[...] = multiply(other, split(middle_ref[...]))


def top_body(assign_ref, got_ref, tail_ref, middle_ref, begun_ref, out_ref):
    half = middle_ref.shape[0] // 2

    @pl.when(side_of(assign_ref) == 0)
    def _():
        other = split(decoded(got_ref[...], tail_ref[...], 0))
        out_ref[...] = begun_ref[...] + multiply(split(middle_ref[0:half, 0:half]), other)

    @pl.when(side_of(assign_ref) != 0)
    def _():
        out_ref[...] = begun_ref[...]


def call(body, shapes, operands, scratch=(), kept=True):
    smem = pl.BlockSpec(memory_space=pltpu.SMEM)
    vmem = pl.BlockSpec(memory_space=pltpu.VMEM)
    whole = [operand.dtype == jnp.int32 for operand in operands]
    operands = [
        operand if scalar else pltpu.with_memory_space_constraint(operand, pltpu.VMEM)
        for operand, scalar in zip(operands, whole)
    ]
    return pl.pallas_call(
        body,
        out_shape=tuple((pltpu.VMEM if kept else jax.ShapeDtypeStruct)(*shape) for shape in shapes),
        in_specs=[smem if scalar else vmem for scalar in whole],
        out_specs=tuple(vmem for _ in shapes),
        scratch_shapes=list(scratch),
        compiler_params=pltpu.CompilerParams(vmem_limit_bytes=GRANT),
    )(*operands)


def paired(grad_out, acts, stat_old, root_old, assign):
    blk_count = lax.axis_size("blk")
    size = stat_old.shape[-1]
    all_tokens = grad_out.shape[0] * lax.axis_size("tok")
    scaling = 1.0 / math.sqrt(all_tokens)
    square = (size, size)
    far = [mask for mask in range(4, blk_count, 4)]
    sent = acts.T
    parts = {}
    for mask in reversed([2] + far):
        parts[mask] = moved(sent, "blk", mask)
    parts[0], grad, warm = stage([sent, grad_out, root_old[0, 0]])
    (stat,) = stage([stat_old[0, 0]])
    for mask in far:
        parts[mask | 2] = moved(parts[mask], "blk", 2)
    grads = [grad, moved(grad_out, "blk", 1)]
    early = mark(parts[0])
    (squared,) = call(squared_body, [(square, jnp.float32)], [warm])
    (fourth,) = call(fourth_body, [(square, jnp.float32)], [assign, squared, *early])
    groups = []
    operands = [assign]
    for masks in ([0, 2] + far[:1], far[1:] + [far[0] | 2], [mask | 2 for mask in far[1:]]):
        own, own_pay, beside, beside_pay = partial_chunk(
            [parts[mask] for mask in masks], grads, scaling
        )
        own_pay, beside_pay = own_pay.astype(jnp.float16), beside_pay.astype(jnp.float16)
        got, got_beside = crossed(own_pay, 0), crossed(beside_pay, 1)
        beside = moved(beside, "blk", 1)
        operands += [own, got.astype(jnp.float32), beside, got_beside.astype(jnp.float32)]
        groups += [masks, [mask | 1 for mask in masks]]
    half = size // 2
    own_root, top, bottom, high, low = call(
        functools.partial(root_body, groups=groups, all_tokens=all_tokens),
        [
            (square, jnp.float32),
            ((half, size), jnp.float32),
            ((half + TAIL, size), jnp.float32),
            (square, jnp.bfloat16),
            (square, jnp.bfloat16),
        ],
        operands + [stat, warm, fourth],
        [pltpu.VMEM(square, jnp.float32)],
    )
    bottom = crossed(bottom.astype(jnp.float16), 0)
    top = crossed(top.astype(jnp.float16), 0)
    (middle,) = call(middle_body, [(square, jnp.float32)], [assign, own_root, high, low])
    begun, tail = call(
        bottom_body,
        [((half, size), jnp.float32), ((TAIL, size), jnp.float32)],
        [assign, bottom.astype(jnp.float32), middle],
    )
    (precond,) = call(
        top_body,
        [((half, size), jnp.float32)],
        [assign, top.astype(jnp.float32), tail, middle, begun],
        kept=False,
    )
    return (own_root[None, None], precond[None, None])


def is_paired(mesh_shape, rows, size, features):
    strips = rows // size
    plain = mesh_shape["tok"] == 2 and strips == mesh_shape["blk"] and strips % 8 == 0
    return plain and features % (32 * strips) == 0


def solution(mesh):
    placed = (
        P("tok", "blk"),
        P("tok", "blk"),
        P("tok", "blk", None, None),
        P("tok", "blk", None, None),
        P("blk", None),
    )

    def whole(grad_out, acts, stat_old, root_old, assign):
        fast = is_paired(mesh.shape, grad_out.shape[1], stat_old.shape[-1], acts.shape[1])

        def shards(*args):
            return (paired if fast else general)(*args)

        mapped = jax.shard_map(
            shards,
            mesh=mesh,
            in_specs=placed,
            out_specs=(P("tok", "blk", None, None), P("tok", "blk", None, None)),
            check_vma=False,
        )
        return mapped(grad_out, acts, stat_old, root_old, assign)

    return whole
```

```python
import functools
import math

import jax
import jax.numpy as jnp
from jax import lax
from jax.experimental import pallas as pl
from jax.experimental.pallas import tpu as pltpu
from jax.sharding import PartitionSpec as P


ITERS = 2


BETA = 0.9
DAMPING = 0.001
TAIL = 8
GRANT = 24 << 20


def swapped(block, axis, stride):
    return moved(block, axis, 1 << stride)


def crossed(block, mask):
    half = lax.axis_size("blk")
    return lax.ppermute(
        block, ("tok", "blk"), [(low, low ^ half ^ mask) for low in range(2 * half)]
    )


def moved(block, axis, mask):
    count = lax.axis_size(axis)
    return lax.ppermute(block, axis, [(low, low ^ mask) for low in range(count) if low ^ mask < count])


def product(lhs_matrix, rhs_matrix):
    return jnp.dot(
        lhs_matrix, rhs_matrix, precision=lax.Precision.HIGH, preferred_element_type=jnp.float32
    )


def newton_root(statistic, warm_root, square):
    identity = jnp.eye(square.shape[0], dtype=jnp.float32)
    factor = BETA * statistic + (1.0 - BETA) * square + DAMPING * identity
    root_square = product(warm_root, warm_root)
    coupled = product(product(root_square, root_square), factor)
    current = warm_root
    for iteration in range(ITERS):
        update = (5.0 * identity - coupled) * 0.25
        current = product(current, update)
        if iteration + 1 < ITERS:
            update_square = product(update, update)
            coupled = product(product(update_square, update_square), coupled)
    return current


def block_partials(rows_part, cols_part, group_blocks, block_size, scaling):
    shaped = cols_part.reshape(cols_part.shape[0], group_blocks, block_size)
    return (
        jnp.einsum("tr,tgc->grc", rows_part, shaped, preferred_element_type=jnp.float32) * scaling
    )


def join_pair(mine, theirs, column, bit):
    lower = column // (1 << bit) % 2 == 0
    return jnp.where(
        lower, jnp.concatenate([mine, theirs], axis=1), jnp.concatenate([theirs, mine], axis=1)
    )


def general(grad_out, acts, stat_old, root_old, assign):
    token_groups = lax.axis_size("tok")
    blk_count = lax.axis_size("blk")
    column = lax.axis_index("blk")
    position = lax.axis_index("tok")
    block_size = stat_old.shape[-1]
    shard_rows = grad_out.shape[0]
    all_tokens = shard_rows * token_groups
    scaling = 1.0 / math.sqrt(all_tokens)
    strips = grad_out.shape[1] * blk_count // block_size
    strip_bits = strips.bit_length() - 1
    blk_bits = blk_count.bit_length() - 1
    group_blocks = token_groups // 2
    cols_part = acts
    for bit in range(strip_bits):
        other_cols = swapped(cols_part, "blk", bit)
        cols_part = join_pair(cols_part, other_cols, column, bit)
    rows_part = grad_out
    for bit in range(strip_bits, blk_bits):
        other_rows = swapped(rows_part, "blk", bit)
        rows_part = join_pair(rows_part, other_rows, column, bit)
    job_table = assign[0]
    job_index = job_table[position]
    side_bit = job_index % 2
    partial_value = block_partials(rows_part, cols_part, group_blocks, block_size, scaling)
    halves = partial_value.reshape(group_blocks * 2, block_size // 2, block_size)[job_table]
    own_half = lax.psum_scatter(halves, "tok", scatter_dimension=0, tiled=True)[0]
    other_half = swapped(own_half, "tok", 0)
    chosen = jnp.where(
        side_bit == 0,
        jnp.concatenate([own_half, other_half], axis=0),
        jnp.concatenate([other_half, own_half], axis=0),
    )
    oriented = jnp.where(side_bit == 0, chosen, chosen.T)
    square = product(oriented, oriented.T) / all_tokens
    own_root = newton_root(stat_old[0, 0], root_old[0, 0], square)
    other_root = swapped(own_root, "tok", 0)
    left_root = jnp.where(side_bit == 0, own_root, other_root)
    right_root = jnp.where(side_bit == 0, other_root, own_root)
    half_rows = lax.dynamic_slice_in_dim(
        left_root, side_bit * (block_size // 2), block_size // 2, 0
    )
    precond = product(product(half_rows, chosen), right_root)
    return (own_root[None, None], precond[None, None])


def split(value):
    high = value.astype(jnp.bfloat16)
    return high, (value - high.astype(jnp.float32)).astype(jnp.bfloat16)


def multiply(lhs, rhs, dims=((1,), (0,))):
    def one(a, b):
        return lax.dot_general(a, b, (dims, ((), ())), preferred_element_type=jnp.float32)

    return one(lhs[0], rhs[0]) + (one(lhs[0], rhs[1]) + one(lhs[1], rhs[0]))


def exponent_of(value):
    largest = jnp.max(jnp.abs(value), axis=0, keepdims=True)
    return jnp.clip(jnp.ceil(jnp.log2(jnp.maximum(largest, 1e-30))), -100.0, 100.0)


def side_of(assign_ref):
    return assign_ref[0, lax.axis_index("tok")] % 2


def eye_mask(rows, cols):
    return lax.broadcasted_iota(jnp.int32, (rows, cols), 0) == lax.broadcasted_iota(
        jnp.int32, (rows, cols), 1
    )


def partial_body(*refs, scaling, pieces):
    grad_refs = refs[pieces : pieces + 2]
    outs = refs[pieces + 2 :]
    held_ref = outs[-1]
    part_rows = refs[0].shape[0]
    rows = pieces * part_rows
    for index in range(pieces):
        held_ref[index * part_rows : (index + 1) * part_rows, :] = refs[index][...]
    for which, grad_ref in enumerate(grad_refs):
        own_ref, pay_ref = outs[2 * which : 2 * which + 2]
        own = jnp.dot(held_ref[...], grad_ref[...], preferred_element_type=jnp.float32) * scaling
        own_ref[...] = own
        power = exponent_of(own)
        pay_ref[0:rows, :] = own * jnp.exp2(-power)
        pay_ref[rows:, :] = jnp.broadcast_to(power, (TAIL, own.shape[1]))


def partial_chunk(parts, grads, scaling):
    rows = sum(part.shape[0] for part in parts)
    width = grads[0].shape[1]
    return call(
        functools.partial(partial_body, scaling=scaling, pieces=len(parts)),
        [((rows, width), jnp.float32), ((rows + TAIL, width), jnp.float32)] * 2,
        [*parts, *grads],
        [pltpu.VMEM((rows, grads[0].shape[0]), grads[0].dtype)],
    )


def stage_body(*refs):
    count = len(refs) // 2
    copies = [
        pltpu.make_async_copy(refs[index], refs[count + index], refs[-1].at[index])
        for index in range(count)
    ]
    for copy in copies:
        copy.start()
    for copy in copies:
        copy.wait()


def stage(operands):
    operands = [pltpu.with_memory_space_constraint(operand, pltpu.HBM) for operand in operands]
    return pl.pallas_call(
        stage_body,
        out_shape=tuple(pltpu.VMEM(operand.shape, operand.dtype) for operand in operands),
        in_specs=[pl.BlockSpec(memory_space=pl.ANY) for _ in operands],
        out_specs=tuple(pl.BlockSpec(memory_space=pltpu.VMEM) for _ in operands),
        scratch_shapes=[pltpu.SemaphoreType.DMA((len(operands),))],
        compiler_params=pltpu.CompilerParams(vmem_limit_bytes=GRANT),
    )(*operands)


def mark_body(block_ref, out_ref):
    out_ref[...] = block_ref[0:8, 0:128].astype(jnp.float32)


def mark(block):
    return call(mark_body, [((8, 128), jnp.float32)], [block])


def squared_body(root_ref, out_ref):
    value = split(root_ref[...])
    out_ref[...] = multiply(value, value)


def fourth_body(assign_ref, squared_ref, early_ref, out_ref):
    value = split(squared_ref[...])
    out_ref[...] = multiply(value, value)


def root_body(*refs, groups, all_tokens):
    assign_ref = refs[0]
    count = len(groups)
    stat_ref, warm_ref, fourth_ref = refs[1 + 2 * count : 4 + 2 * count]
    root_ref, top_ref, bottom_ref, high_ref, low_ref, held_ref = refs[4 + 2 * count :]
    column, side = lax.axis_index("blk"), side_of(assign_ref)
    size = stat_ref.shape[-1]
    for group, masks in enumerate(groups):
        own_ref, got_ref = refs[1 + 2 * group : 3 + 2 * group]
        rows = own_ref.shape[0]
        part_rows = rows // len(masks)
        scale = jnp.exp2(got_ref[rows : rows + 1, :])
        for index, mask in enumerate(masks):
            span = slice(index * part_rows, (index + 1) * part_rows)
            target = pl.multiple_of((column ^ mask) * part_rows, part_rows)
            held_ref[pl.ds(target, part_rows), :] = own_ref[span, :] + got_ref[span, :] * scale

    @pl.when(side == 0)
    def _():
        held_ref[...] = held_ref[...].T

    oriented = split(held_ref[...])
    high_ref[...] = oriented[0]
    low_ref[...] = oriented[1]
    square = multiply(oriented, oriented, ((1,), (1,))) * (1.0 / all_tokens)
    identity = jnp.where(eye_mask(size, size), 1.0, 0.0)
    factor = BETA * stat_ref[...] + (1.0 - BETA) * square + DAMPING * identity
    coupled = multiply(split(fourth_ref[...]), split(factor))
    update = (5.0 * identity - coupled) * 0.25
    parts = split(update)
    update_square = multiply(parts, parts)
    parts = split(update_square)
    update_fourth = split(multiply(parts, parts))
    inner = split(4.0 * update_square - 5.0 * update)
    both_steps = (5.0 * update + multiply(update_fourth, inner)) * 0.25
    current = multiply(split(warm_ref[...]), split(both_steps))
    root_ref[...] = current
    power = exponent_of(current)
    scaled = current * jnp.exp2(-power)
    diagonal = jnp.sum(scaled * identity, axis=0, keepdims=True)
    coarse = jnp.round(diagonal * 1024.0) * (1.0 / 1024.0)
    half = size // 2
    scaled = scaled * (1.0 - identity)
    top_ref[...] = scaled[:half, :]
    bottom_ref[0:half, :] = scaled[half:, :]
    row = lax.broadcasted_iota(jnp.int32, (TAIL, size), 0)
    tail = jnp.where(row == 0, power, jnp.where(row == 1, coarse, diagonal - coarse))
    bottom_ref[half:, :] = tail


def middle_body(assign_ref, root_ref, high_ref, low_ref, out_high_ref, out_low_ref):
    half = root_ref.shape[0] // 2
    oriented = high_ref[...], low_ref[...]

    @pl.when(side_of(assign_ref) == 0)
    def _():
        held = split(multiply(split(root_ref[0:half, :]), oriented))
        out_high_ref[0:half, :], out_low_ref[0:half, :] = held
        out_high_ref[half:, :] = jnp.zeros((half, root_ref.shape[1]), jnp.bfloat16)
        out_low_ref[half:, :] = jnp.zeros((half, root_ref.shape[1]), jnp.bfloat16)

    @pl.when(side_of(assign_ref) != 0)
    def _():
        out_high_ref[...], out_low_ref[...] = split(
            multiply(oriented, split(root_ref[...]), ((0,), (0,)))
        )


def decoded(rows, tail, offset):
    mask = lax.broadcasted_iota(jnp.int32, rows.shape, 0) + offset == lax.broadcasted_iota(
        jnp.int32, rows.shape, 1
    )
    return jnp.where(mask, tail[1:2, :] + tail[2:3, :], rows) * jnp.exp2(tail[0:1, :])


def bottom_body(assign_ref, got_ref, high_ref, low_ref, out_ref, tail_ref):
    half = high_ref.shape[0] // 2
    tail = got_ref[half:, :]
    tail_ref[...] = tail
    other = split(decoded(got_ref[0:half, :], tail, half))

    @pl.when(side_of(assign_ref) == 0)
    def _():
        out_ref[...] = multiply((high_ref[0:half, half:], low_ref[0:half, half:]), other)

    @pl.when(side_of(assign_ref) != 0)
    def _():
        out_ref[...] = multiply(other, (high_ref[...], low_ref[...]))


def top_body(assign_ref, got_ref, tail_ref, high_ref, low_ref, begun_ref, out_ref):
    half = high_ref.shape[0] // 2

    @pl.when(side_of(assign_ref) == 0)
    def _():
        other = split(decoded(got_ref[...], tail_ref[...], 0))
        out_ref[...] = begun_ref[...] + multiply((high_ref[0:half, 0:half], low_ref[0:half, 0:half]), other)

    @pl.when(side_of(assign_ref) != 0)
    def _():
        out_ref[...] = begun_ref[...]


def call(body, shapes, operands, scratch=(), kept=True):
    smem = pl.BlockSpec(memory_space=pltpu.SMEM)
    vmem = pl.BlockSpec(memory_space=pltpu.VMEM)
    whole = [operand.dtype == jnp.int32 for operand in operands]
    operands = [
        operand if scalar else pltpu.with_memory_space_constraint(operand, pltpu.VMEM)
        for operand, scalar in zip(operands, whole)
    ]
    return pl.pallas_call(
        body,
        out_shape=tuple((pltpu.VMEM if kept else jax.ShapeDtypeStruct)(*shape) for shape in shapes),
        in_specs=[smem if scalar else vmem for scalar in whole],
        out_specs=tuple(vmem for _ in shapes),
        scratch_shapes=list(scratch),
        compiler_params=pltpu.CompilerParams(vmem_limit_bytes=GRANT),
    )(*operands)


def paired(grad_out, acts, stat_old, root_old, assign):
    blk_count = lax.axis_size("blk")
    size = stat_old.shape[-1]
    all_tokens = grad_out.shape[0] * lax.axis_size("tok")
    scaling = 1.0 / math.sqrt(all_tokens)
    square = (size, size)
    far = [mask for mask in range(4, blk_count, 4)]
    sent = acts.T
    parts = {}
    for mask in reversed([2] + far):
        parts[mask] = moved(sent, "blk", mask)
    parts[0], grad, warm = stage([sent, grad_out, root_old[0, 0]])
    (stat,) = stage([stat_old[0, 0]])
    for mask in far:
        parts[mask | 2] = moved(parts[mask], "blk", 2)
    grads = [grad, moved(grad_out, "blk", 1)]
    early = mark(parts[0])
    (squared,) = call(squared_body, [(square, jnp.float32)], [warm])
    (fourth,) = call(fourth_body, [(square, jnp.float32)], [assign, squared, *early])
    groups = []
    operands = [assign]
    for masks in ([0, 2] + far[:1], far[1:] + [far[0] | 2], [mask | 2 for mask in far[1:]]):
        own, own_pay, beside, beside_pay = partial_chunk(
            [parts[mask] for mask in masks], grads, scaling
        )
        own_pay, beside_pay = own_pay.astype(jnp.float16), beside_pay.astype(jnp.float16)
        got, got_beside = crossed(own_pay, 0), crossed(beside_pay, 1)
        beside = moved(beside, "blk", 1)
        operands += [own, got.astype(jnp.float32), beside, got_beside.astype(jnp.float32)]
        groups += [masks, [mask | 1 for mask in masks]]
    half = size // 2
    own_root, top, bottom, high, low = call(
        functools.partial(root_body, groups=groups, all_tokens=all_tokens),
        [
            (square, jnp.float32),
            ((half, size), jnp.float32),
            ((half + TAIL, size), jnp.float32),
            (square, jnp.bfloat16),
            (square, jnp.bfloat16),
        ],
        operands + [stat, warm, fourth],
        [pltpu.VMEM(square, jnp.float32)],
    )
    bottom = crossed(bottom.astype(jnp.float16), 0)
    top = crossed(top.astype(jnp.float16), 0)
    middle = call(middle_body, [(square, jnp.bfloat16)] * 2, [assign, own_root, high, low])
    begun, tail = call(
        bottom_body,
        [((half, size), jnp.float32), ((TAIL, size), jnp.float32)],
        [assign, bottom.astype(jnp.float32), *middle],
    )
    (precond,) = call(
        top_body,
        [((half, size), jnp.float32)],
        [assign, top.astype(jnp.float32), tail, *middle, begun],
        kept=False,
    )
    return (own_root[None, None], precond[None, None])


def is_paired(mesh_shape, rows, size, features):
    strips = rows // size
    plain = mesh_shape["tok"] == 2 and strips == mesh_shape["blk"] and strips % 8 == 0
    return plain and features % (32 * strips) == 0


def solution(mesh):
    placed = (
        P("tok", "blk"),
        P("tok", "blk"),
        P("tok", "blk", None, None),
        P("tok", "blk", None, None),
        P("blk", None),
    )

    def whole(grad_out, acts, stat_old, root_old, assign):
        fast = is_paired(mesh.shape, grad_out.shape[1], stat_old.shape[-1], acts.shape[1])

        def shards(*args):
            return (paired if fast else general)(*args)

        mapped = jax.shard_map(
            shards,
            mesh=mesh,
            in_specs=placed,
            out_specs=(P("tok", "blk", None, None), P("tok", "blk", None, None)),
            check_vma=False,
        )
        return mapped(grad_out, acts, stat_old, root_old, assign)

    return whole
```
